32 devices in a mesh: row: 4 (over z), col: 8 (over y, x, core).
Axes of the slice: x: 2, y: 2, z: 4, core: 2. Of those that a mesh axis runs over, the one named last changes fastest.
Arguments:
- front_matrix: bfloat16 [32768, 32768], P('row', 'col'), may hold values from -0.03125 to 0.03125
- right_random: bfloat16 [32768, 128], P(('col', 'row')), may hold values from -32 to 32
- left_random: bfloat16 [32768, 128], P(('row', 'col')), may hold values from -32 to 32
- row_basis: bfloat16 [32768, 384], P('row'), may hold values from -1 to 1, as said below
- column_basis: bfloat16 [32768, 384], P('col'), may hold values from -1 to 1, as said below
Outputs:
- row_samples: float32 [128, 32768], P('col', 'row')
- column_samples: float32 [128, 32768], P('row', 'col')
- row_spread: float32 [64], P('row')
- column_spread: float32 [64], P('col')
The draws below stay inside these ranges and needn't reach their ends.
Inputs may be any that keep to these rules, and one draw needn't show every extreme that they name: Within each leaf node's 512 rows, the columns of row_basis are orthonormal up to their rounding to bfloat16. Within each leaf node's 512 rows, the columns of column_basis are orthonormal up to their rounding to bfloat16.
All inputs are finite; a program needn't handle non-finite values.
Results may differ from the reference program's by a relative error of at most 0.0003.
Values may be sent and summed in bfloat16 or wider, within the bound.
A program may use at most 128 MiB of HBM per device.

```python
import jax
import jax.numpy as jnp
from jax import lax

N = 32768
SAMPLES = 128
EARLIER = 384
NODE = 512


def node_orthonormal(key):
    normals = jax.random.normal(key, (N // NODE, NODE, EARLIER), jnp.float32)
    factors, _ = jnp.linalg.qr(normals)
    return factors.reshape(N, EARLIER).astype(jnp.bfloat16)


def rising_block(key):
    position = jnp.arange(SAMPLES, dtype=jnp.float32) / (SAMPLES - 1)
    entries = jnp.clip(jax.random.normal(key, (N, SAMPLES), jnp.float32), -4.0, 4.0)
    scales = jnp.exp(position * jnp.log(4.0))
    return (entries * scales[None, :]).astype(jnp.bfloat16)


def draw_right_random(key, part):
    return rising_block(jax.random.fold_in(key, 41))


def draw_left_random(key, part):
    return rising_block(jax.random.fold_in(key, 53))


def draw_row_basis(key, part):
    return node_orthonormal(jax.random.fold_in(key, 11))


def draw_column_basis(key, part):
    return node_orthonormal(jax.random.fold_in(key, 29))


def block_scale(own_key, dims, cuts, smallest, high):
    def one(dim, blocks):
        draws = jax.random.uniform(jax.random.fold_in(jax.random.fold_in(own_key, 6), dim), (blocks,), jnp.float32, smallest / len(cuts), high / len(cuts))
        return jnp.repeat(jnp.exp(draws), dims[dim] // blocks).reshape((-1,) + (1,) * (len(dims) - dim - 1))

    loudness = one(*cuts[0])
    for cut in cuts[1:]:
        loudness = loudness * one(*cut)
    return loudness


def normal_values(key, dims, spread, reach, pieces=(), held_as=jnp.bfloat16):
    drawn = spread * jax.random.normal(key, dims, jnp.float32)
    if pieces:
        drawn = drawn * block_scale(key, dims, pieces, -0.22, 0.18)
    return jnp.clip(drawn, -reach, reach).astype(held_as)


def setup_inputs(seed: int = 0) -> dict:
    splits = jax.random.split(jax.random.key(seed), 6)
    front_matrix = normal_values(splits[0], (N, N), N ** -0.5, 0.03125, ((0, 4), (1, 8)))
    right_random = draw_right_random(jax.random.fold_in(splits[5], 71), 0)
    left_random = draw_left_random(jax.random.fold_in(splits[5], 71), 0)
    row_basis = draw_row_basis(jax.random.fold_in(splits[5], 71), 0)
    column_basis = draw_column_basis(jax.random.fold_in(splits[5], 71), 0)
    return {"front_matrix": front_matrix, "right_random": right_random, "left_random": left_random, "row_basis": row_basis, "column_basis": column_basis}


def project_out(full_samples, basis):
    count = full_samples.shape[0]
    nodes = basis.shape[0] // NODE
    shaped = full_samples.astype(jnp.float32).reshape(count, nodes, NODE)
    stacked = basis.astype(jnp.float32).reshape(nodes, NODE, EARLIER)
    coeffs = jnp.einsum('knr,nre->kne', shaped, stacked, precision=lax.Precision.HIGHEST)
    correction = jnp.einsum('kne,nre->knr', coeffs, stacked, precision=lax.Precision.HIGHEST)
    cleaned = shaped - correction
    squares = lax.optimization_barrier(jnp.sum(cleaned * cleaned, axis=(0, 2)))
    return (cleaned.reshape(count, nodes * NODE), jnp.sqrt(squares / (SAMPLES * NODE)))

def reference(front_matrix, right_random, left_random, row_basis, column_basis):
    row_full = jnp.dot(front_matrix.astype(jnp.float32), right_random.astype(jnp.float32), preferred_element_type=jnp.float32).T
    column_full = jnp.dot(left_random.T.astype(jnp.float32), front_matrix.astype(jnp.float32), preferred_element_type=jnp.float32)
    row_samples, row_spread = project_out(row_full, row_basis)
    column_samples, column_spread = project_out(column_full, column_basis)
    return (row_samples, column_samples, row_spread, column_spread)
```

```python
import functools

import jax
import jax.numpy as jnp
from jax import lax
from jax.experimental import pallas as pl
from jax.experimental.pallas import tpu as pltpu
from jax.sharding import PartitionSpec as P

NODE = 512
BUFS = 3
MESH = pl.DeviceIdType.MESH
F32 = jnp.float32
BF16 = jnp.bfloat16


def split3(x):
    hi = x.astype(BF16)
    rest = x - hi.astype(F32)
    mid = rest.astype(BF16)
    lo = (rest - mid.astype(F32)).astype(BF16)
    return hi, mid, lo


def times_basis(x, basis, dims):
    parts = split3(x)
    s = x.shape[0]
    if s % 16 == 0:
        y = lax.dot_general(jnp.concatenate(parts, axis=0), basis, (dims, ((), ())), preferred_element_type=F32)
        return y[:s] + (y[s:2 * s] + y[2 * s:])
    ys = [lax.dot_general(p, basis, (dims, ((), ())), preferred_element_type=F32) for p in parts]
    return ys[0] + (ys[1] + ys[2])


def project(x, basis):
    coeffs = times_basis(x, basis, ((1,), (0,)))
    return x - times_basis(coeffs, basis, ((1,), (1,)))


def kernel(nrow, ncol, front, right, left, rbasis, cbasis,
           row_out, col_out, rspread, cspread,
           leftbuf, rightbuf, cblk, rblk, acc, crecv, stage, precv, rsum, rchip,
           rb, cb, rsq, csq, rsqbuf, csqbuf,
           lsend, lrecv, gsend, grecv, csend, crsem, psend, prsem, xsend, xrsem,
           ssend, srrecv, screcv, local, bsem, cfsem, rfsem):
    r = lax.axis_index("row")
    c = lax.axis_index("col")
    rows, cols = front.shape
    samples = right.shape[1]
    nchip = ncol // 2
    chip, core = lax.div(c, 2), lax.rem(c, 2)
    partner = lax.bitwise_xor(c, 1)
    kb, half = rows // ncol, cols // 2
    steps = 2 * ncol
    panels = rows // NODE
    cnodes = cols // NODE
    sr, sc = samples // ncol, samples // nrow

    def cfetch(i):
        s, h = lax.rem(i, ncol), lax.div(i, ncol)
        k = lax.bitwise_xor(c, s)
        slot = lax.rem(i, BUFS)
        return pltpu.make_async_copy(
            front.at[pl.ds(pl.multiple_of(k * kb, kb), kb), pl.ds(pl.multiple_of(h * half, half), half)],
            cblk.at[slot], cfsem.at[slot])

    def rfetch(p):
        slot = lax.rem(p, BUFS)
        return pltpu.make_async_copy(front.at[pl.ds(pl.multiple_of(p * NODE, NODE), NODE), :], rblk.at[slot], rfsem.at[slot])

    def lcopy(src, slot, dev):
        return pltpu.make_async_remote_copy(src, leftbuf.at[slot], lsend, lrecv.at[slot], device_id={"col": dev}, device_id_type=MESH)

    def gcopy(slot, dev):
        return pltpu.make_async_remote_copy(right, rightbuf.at[slot], gsend, grecv.at[slot], device_id={"row": dev}, device_id_type=MESH)

    def ccopy(h, block, slot, dev):
        return pltpu.make_async_remote_copy(acc.at[h, block], crecv.at[h, slot], csend, crsem.at[h, slot], device_id={"row": dev}, device_id_type=MESH)

    def pcopy(p):
        return pltpu.make_async_remote_copy(stage.at[p, 1 - core], precv.at[p], psend, prsem.at[p], device_id={"col": partner}, device_id_type=MESH)

    def xcopy(p, block, slot, dev):
        return pltpu.make_async_remote_copy(rsum.at[p, block], rchip.at[p, slot], xsend, xrsem.at[p, slot], device_id={"col": dev}, device_id_type=MESH)

    for i in range(BUFS - 1):
        cfetch(jnp.int32(i)).start()
    own_left = pltpu.make_async_copy(left, leftbuf.at[c], local.at[0])
    own_right = pltpu.make_async_copy(right, rightbuf.at[r], local.at[1])
    own_left.start()
    own_right.start()

    barrier = pltpu.get_barrier_semaphore()
    for s in range(1, ncol):
        pl.semaphore_signal(barrier, inc=1, device_id={"col": lax.bitwise_xor(c, s)}, device_id_type=MESH)
    for t in range(1, nrow):
        pl.semaphore_signal(barrier, inc=1, device_id={"row": lax.bitwise_xor(r, t)}, device_id_type=MESH)
    acc[...] = jnp.zeros_like(acc)
    rsq[...] = jnp.zeros_like(rsq)
    csq[...] = jnp.zeros_like(csq)
    pl.semaphore_wait(barrier, ncol - 1 + nrow - 1)

    lcopy(left, c, partner).start()
    for j in range(1, nchip):
        lcopy(left, c, lax.bitwise_xor(c, 2 * j)).start()
    for t in range(1, nrow):
        gcopy(r, lax.bitwise_xor(r, t)).start()
    bases = (pltpu.make_async_copy(rbasis, rb, bsem.at[0]), pltpu.make_async_copy(cbasis, cb, bsem.at[1]))
    own_left.wait()

    @pl.loop(0, steps)
    def _(i):
        s, h = lax.rem(i, ncol), lax.div(i, ncol)
        k = lax.bitwise_xor(c, s)
        slot = lax.rem(i, BUFS)

        @pl.when(i + BUFS - 1 < steps)
        def _():
            cfetch(i + BUFS - 1).start()

        @pl.when(i + BUFS - 1 >= steps)
        def _():
            rfetch(i + BUFS - 1 - steps).start()

        @pl.when(i == ncol)
        def _():
            for b in bases:
                b.start()

        @pl.when((i > 0) & (i < ncol))
        def _():
            lcopy(left, k, partner).wait_recv()

        @pl.when((i > 1) & (i < ncol) & (lax.rem(i, 2) == 0))
        def _():
            lcopy(leftbuf.at[k], k, partner).start()

        cfetch(i).wait()
        lt = leftbuf[k].T
        width = min(NODE, half)
        for n in range(half // width):
            piece = jnp.dot(lt, cblk[slot, :, n * width:(n + 1) * width], preferred_element_type=F32)
            acc[h, :, :, n * width:(n + 1) * width] += piece.reshape(nrow, sc, width)

        @pl.when(s == ncol - 1)
        def _():
            for t in range(1, nrow):
                peer = lax.bitwise_xor(r, t)
                ccopy(h, peer, r, peer).start()

    own_right.wait()
    for t in range(1, nrow):
        gcopy(lax.bitwise_xor(r, t), r).wait_recv()

    def reduce(p):
        pcopy(p).wait_recv()
        both = stage[p, core] + precv[p]
        rsum[p] = both
        for j in range(1, nchip):
            peer = lax.bitwise_xor(chip, j)
            xcopy(p, peer, chip, peer * 2 + core).start()
        rchip[p, chip] = rsum[p, chip]

    @pl.loop(0, panels)
    def _(p):
        slot = lax.rem(p, BUFS)

        @pl.when(p + BUFS - 1 < panels)
        def _():
            rfetch(p + BUFS - 1).start()

        rfetch(p).wait()
        g = rightbuf[...].reshape(cols, samples)
        res = jnp.dot(rblk[slot], g, preferred_element_type=F32).T
        for d in range(ncol):
            stage[p, d % 2, d // 2] = res[d * sr:(d + 1) * sr]
        pcopy(p).start()

        @pl.when(p > 0)
        def _():
            reduce(p - 1)

    reduce(jnp.int32(panels - 1))
    for b in bases:
        b.wait()

    lane = lax.broadcasted_iota(jnp.int32, rsq.shape, 1)
    per = cnodes // 2
    for h in range(2):
        for t in range(1, nrow):
            peer = lax.bitwise_xor(r, t)
            ccopy(h, r, peer, peer).wait_recv()
        crecv[h, r] = acc[h, r]
        for q in range(per):
            n = h * per + q
            x = crecv[h, 0, :, q * NODE:(q + 1) * NODE]
            for t in range(1, nrow):
                x = x + crecv[h, t, :, q * NODE:(q + 1) * NODE]
            y = project(x, cb[n * NODE:(n + 1) * NODE, :])
            col_out[:, n * NODE:(n + 1) * NODE] = y
            csq[...] = jnp.where(lane == n, jnp.sum(y * y), csq[...])
    csqbuf[r] = csq[...]

    def scopy(t):
        peer = lax.bitwise_xor(r, t)
        return pltpu.make_async_remote_copy(csq, csqbuf.at[r], ssend, screcv.at[r], device_id={"row": peer}, device_id_type=MESH)

    for t in range(1, nrow):
        scopy(t).start()

    unroll = 4 if panels % 4 == 0 else 1

    @pl.loop(0, panels // unroll)
    def _(b):
        for u in range(unroll):
            p = b * unroll + u
            for j in range(1, nchip):
                peer = lax.bitwise_xor(chip, j)
                xcopy(p, chip, peer, peer * 2 + core).wait_recv()
        for u in range(unroll):
            p = b * unroll + u
            x = rchip[p, 0]
            for j in range(1, nchip):
                x = x + rchip[p, j]
            where = pl.ds(pl.multiple_of(p * NODE, NODE), NODE)
            y = project(x, rb[where, :])
            row_out[:, where] = y
            rsq[...] = jnp.where(lane == p, jnp.sum(y * y), rsq[...])

    rsqbuf[c] = rsq[...]

    def tcopy(s):
        peer = lax.bitwise_xor(c, s)
        return pltpu.make_async_remote_copy(rsq, rsqbuf.at[c], ssend, srrecv.at[c], device_id={"col": peer}, device_id_type=MESH)

    for s in range(1, ncol):
        tcopy(s).start()

    def wait_slot(src, buf, sems, slot, dev):
        pltpu.make_async_remote_copy(src, buf.at[slot], ssend, sems.at[slot], device_id=dev, device_id_type=MESH).wait_recv()

    lcopy(left, c, partner).wait_send()
    for j in range(1, nchip):
        lcopy(left, c, partner).wait_send()
        lcopy(leftbuf.at[c], c, partner).wait_send()
    for t in range(1, nrow):
        gcopy(r, r).wait_send()
        for h in range(2):
            ccopy(h, r, r, r).wait_send()

    @pl.loop(0, panels)
    def _(p):
        pcopy(p).wait_send()
        for j in range(1, nchip):
            xcopy(p, chip, chip, c).wait_send()

    for t in range(1, nrow):
        peer = lax.bitwise_xor(r, t)
        wait_slot(csq, csqbuf, screcv, peer, {"row": peer})
    for s in range(1, ncol):
        peer = lax.bitwise_xor(c, s)
        wait_slot(rsq, rsqbuf, srrecv, peer, {"col": peer})
    count = samples * NODE
    total = rsqbuf[0]
    for s in range(1, ncol):
        total = total + rsqbuf[s]
    rspread[...] = jnp.sqrt(total / count)
    total = csqbuf[0]
    for t in range(1, nrow):
        total = total + csqbuf[t]
    cspread[...] = jnp.sqrt(total / count)
    for t in range(1, nrow):
        scopy(t).wait_send()
    for s in range(1, ncol):
        tcopy(s).wait_send()


def shards(nrow, ncol, front, right, left, row_basis, column_basis):
    rows, cols = front.shape
    samples = right.shape[1]
    early = row_basis.shape[1]
    nchip = ncol // 2
    sr, sc = samples // ncol, samples // nrow
    panels = rows // NODE
    half = cols // 2
    dma = pltpu.SemaphoreType.DMA
    hbm = pl.BlockSpec(memory_space=pl.ANY)
    vmem = pl.BlockSpec(memory_space=pltpu.VMEM)
    row_s, col_s, rs, cs = pl.pallas_call(
        functools.partial(kernel, nrow, ncol),
        out_shape=(
            jax.ShapeDtypeStruct((sr, rows), F32),
            jax.ShapeDtypeStruct((sc, cols), F32),
            jax.ShapeDtypeStruct((8, 128), F32),
            jax.ShapeDtypeStruct((8, 128), F32),
        ),
        in_specs=[hbm] * 5,
        out_specs=(vmem,) * 4,
        scratch_shapes=[
            pltpu.VMEM((ncol,) + left.shape, BF16),
            pltpu.VMEM((nrow,) + right.shape, BF16),
            pltpu.VMEM((BUFS, rows // ncol, half), BF16),
            pltpu.VMEM((BUFS, NODE, cols), BF16),
            pltpu.VMEM((2, nrow, sc, half), F32),
            pltpu.VMEM((2, nrow, sc, half), F32),
            pltpu.VMEM((panels, 2, nchip, sr, NODE), F32),
            pltpu.VMEM((panels, nchip, sr, NODE), F32),
            pltpu.VMEM((panels, nchip, sr, NODE), F32),
            pltpu.VMEM((panels, nchip, sr, NODE), F32),
            pltpu.VMEM((rows, early), BF16),
            pltpu.VMEM((cols, early), BF16),
            pltpu.VMEM((8, 128), F32),
            pltpu.VMEM((8, 128), F32),
            pltpu.VMEM((ncol, 8, 128), F32),
            pltpu.VMEM((nrow, 8, 128), F32),
            dma, dma((ncol,)), dma, dma((nrow,)), dma, dma((2, nrow)),
            dma, dma((panels,)), dma, dma((panels, nchip)),
            dma, dma((ncol,)), dma((nrow,)), dma((2,)), dma((2,)), dma((BUFS,)), dma((BUFS,)),
        ],
        compiler_params=pltpu.CompilerParams(
            collective_id=0, has_side_effects=True, vmem_limit_bytes=62 * 1024 * 1024
        ),
    )(front, right, left, row_basis, column_basis)
    return row_s, col_s, rs[0, :rows // NODE], cs[0, :cols // NODE]


def solution(mesh):
    in_specs = (
        P("row", "col"),
        P(("col", "row"), None),
        P(("row", "col"), None),
        P("row", None),
        P("col", None),
    )
    out_specs = (P("col", "row"), P("row", "col"), P("row"), P("col"))
    body = functools.partial(shards, mesh.shape["row"], mesh.shape["col"])
    return jax.shard_map(body, mesh=mesh, in_specs=in_specs, out_specs=out_specs, check_vma=False)
```

```python
import functools

import jax
import jax.numpy as jnp
from jax import lax
from jax.experimental import pallas as pl
from jax.experimental.pallas import tpu as pltpu
from jax.sharding import PartitionSpec as P

NODE = 512
BUFS = 3
MESH = pl.DeviceIdType.MESH
F32 = jnp.float32
BF16 = jnp.bfloat16


def split3(x):
    hi = x.astype(BF16)
    rest = x - hi.astype(F32)
    mid = rest.astype(BF16)
    lo = (rest - mid.astype(F32)).astype(BF16)
    return hi, mid, lo


def times_basis(x, basis, dims):
    parts = split3(x)
    s = x.shape[0]
    if s % 16 == 0:
        y = lax.dot_general(jnp.concatenate(parts, axis=0), basis, (dims, ((), ())), preferred_element_type=F32)
        return y[:s] + (y[s:2 * s] + y[2 * s:])
    ys = [lax.dot_general(p, basis, (dims, ((), ())), preferred_element_type=F32) for p in parts]
    return ys[0] + (ys[1] + ys[2])


def project(xs, bases):
    coeffs = [times_basis(x, b, ((1,), (0,))) for x, b in zip(xs, bases)]
    return [x - times_basis(k, b, ((1,), (1,))) for x, k, b in zip(xs, coeffs, bases)]


def kernel(nrow, ncol, front, right, left, rbasis, cbasis,
           row_out, col_out, rspread, cspread,
           leftbuf, rightbuf, cblk, rblk, acc, crecv, stage, precv, rsum, rchip,
           rb, cb, rsq, csq, rsqbuf, csqbuf,
           lsend, lrecv, gsend, grecv, csend, crsem, psend, prsem, xsend, xrsem,
           ssend, srrecv, screcv, local, bsem, cfsem, rfsem):
    r = lax.axis_index("row")
    c = lax.axis_index("col")
    rows, cols = front.shape
    samples = right.shape[1]
    nchip = ncol // 2
    chip, core = lax.div(c, 2), lax.rem(c, 2)
    partner = lax.bitwise_xor(c, 1)
    kb, half = rows // ncol, cols // 2
    steps = 2 * ncol
    panels = rows // NODE
    cnodes = cols // NODE
    sr, sc = samples // ncol, samples // nrow

    def order(i):
        j = i - 4
        early = i < 4
        s = jnp.where(early, lax.div(i, 2), 2 + lax.rem(jnp.maximum(j, 0), ncol - 2))
        h = jnp.where(early, lax.rem(i, 2), lax.div(jnp.maximum(j, 0), ncol - 2))
        return s, h

    def cfetch(i):
        s, h = order(i)
        k = lax.bitwise_xor(c, s)
        slot = lax.rem(i, BUFS)
        return pltpu.make_async_copy(
            front.at[pl.ds(pl.multiple_of(k * kb, kb), kb), pl.ds(pl.multiple_of(h * half, half), half)],
            cblk.at[slot], cfsem.at[slot])

    def rfetch(p):
        slot = lax.rem(p, BUFS)
        return pltpu.make_async_copy(front.at[pl.ds(pl.multiple_of(p * NODE, NODE), NODE), :], rblk.at[slot], rfsem.at[slot])

    def lcopy(src, slot, dev):
        return pltpu.make_async_remote_copy(src, leftbuf.at[slot], lsend, lrecv.at[slot], device_id={"col": dev}, device_id_type=MESH)

    def gcopy(slot, dev):
        return pltpu.make_async_remote_copy(right, rightbuf.at[slot], gsend, grecv.at[slot], device_id={"row": dev}, device_id_type=MESH)

    def ccopy(h, block, slot, dev):
        return pltpu.make_async_remote_copy(acc.at[h, block], crecv.at[h, slot], csend, crsem.at[h, slot], device_id={"row": dev}, device_id_type=MESH)

    def pcopy(p):
        return pltpu.make_async_remote_copy(stage.at[p, 1 - core], precv.at[p], psend, prsem.at[p], device_id={"col": partner}, device_id_type=MESH)

    def xcopy(p, block, slot, dev):
        return pltpu.make_async_remote_copy(rsum.at[p, block], rchip.at[p, slot], xsend, xrsem.at[p, slot], device_id={"col": dev}, device_id_type=MESH)

    for i in range(BUFS - 1):
        cfetch(jnp.int32(i)).start()
    own_left = pltpu.make_async_copy(left, leftbuf.at[c], local.at[0])
    own_right = pltpu.make_async_copy(right, rightbuf.at[r], local.at[1])
    own_left.start()
    own_right.start()

    barrier = pltpu.get_barrier_semaphore()
    for s in range(1, ncol):
        pl.semaphore_signal(barrier, inc=1, device_id={"col": lax.bitwise_xor(c, s)}, device_id_type=MESH)
    for t in range(1, nrow):
        pl.semaphore_signal(barrier, inc=1, device_id={"row": lax.bitwise_xor(r, t)}, device_id_type=MESH)
    acc[...] = jnp.zeros_like(acc)
    rsq[...] = jnp.zeros_like(rsq)
    csq[...] = jnp.zeros_like(csq)
    pl.semaphore_wait(barrier, ncol - 1 + nrow - 1)

    lcopy(left, c, partner).start()
    for j in range(1, nchip):
        lcopy(left, c, lax.bitwise_xor(c, 2 * j)).start()
    for t in range(1, nrow):
        gcopy(r, lax.bitwise_xor(r, t)).start()
    bases = (pltpu.make_async_copy(rbasis, rb, bsem.at[0]), pltpu.make_async_copy(cbasis, cb, bsem.at[1]))
    own_left.wait()

    @pl.loop(0, steps)
    def _(i):
        s, h = order(i)
        k = lax.bitwise_xor(c, s)
        slot = lax.rem(i, BUFS)

        @pl.when(i + BUFS - 1 < steps)
        def _():
            cfetch(i + BUFS - 1).start()

        @pl.when(i + BUFS - 1 >= steps)
        def _():
            rfetch(i + BUFS - 1 - steps).start()

        @pl.when(i == ncol)
        def _():
            for b in bases:
                b.start()

        @pl.when((h == 0) & (s > 0))
        def _():
            lcopy(left, k, partner).wait_recv()

        @pl.when((h == 0) & (s > 1) & (lax.rem(s, 2) == 0))
        def _():
            lcopy(leftbuf.at[k], k, partner).start()

        cfetch(i).wait()
        lt = leftbuf[k].T
        width = min(NODE, half)
        for n in range(half // width):
            piece = jnp.dot(lt, cblk[slot, :, n * width:(n + 1) * width], preferred_element_type=F32)
            acc[h, :, :, n * width:(n + 1) * width] += piece.reshape(nrow, sc, width)

        @pl.when(s == ncol - 1)
        def _():
            for t in range(1, nrow):
                peer = lax.bitwise_xor(r, t)
                ccopy(h, peer, r, peer).start()

    own_right.wait()
    for t in range(1, nrow):
        gcopy(lax.bitwise_xor(r, t), r).wait_recv()

    def reduce(p):
        pcopy(p).wait_recv()
        both = stage[p, core] + precv[p]
        rsum[p] = both
        for j in range(1, nchip):
            peer = lax.bitwise_xor(chip, j)
            xcopy(p, peer, chip, peer * 2 + core).start()
        rchip[p, chip] = rsum[p, chip]

    @pl.loop(0, panels)
    def _(p):
        slot = lax.rem(p, BUFS)

        @pl.when(p + BUFS - 1 < panels)
        def _():
            rfetch(p + BUFS - 1).start()

        rfetch(p).wait()
        g = rightbuf[...].reshape(cols, samples)
        res = jnp.dot(rblk[slot], g, preferred_element_type=F32).T
        for d in range(ncol):
            stage[p, d % 2, d // 2] = res[d * sr:(d + 1) * sr]
        pcopy(p).start()

        @pl.when(p > 0)
        def _():
            reduce(p - 1)

    reduce(jnp.int32(panels - 1))
    for b in bases:
        b.wait()

    lane = lax.broadcasted_iota(jnp.int32, rsq.shape, 1)
    per = cnodes // 2
    for h in range(2):
        for t in range(1, nrow):
            peer = lax.bitwise_xor(r, t)
            ccopy(h, r, peer, peer).wait_recv()
        crecv[h, r] = acc[h, r]
        xs, marks = [], csq[...]
        for q in range(per):
            x = crecv[h, 0, :, q * NODE:(q + 1) * NODE]
            for t in range(1, nrow):
                x = x + crecv[h, t, :, q * NODE:(q + 1) * NODE]
            xs.append(x)
        ys = project(xs, [cb[(h * per + q) * NODE:(h * per + q + 1) * NODE, :] for q in range(per)])
        for q, y in enumerate(ys):
            n = h * per + q
            col_out[:, n * NODE:(n + 1) * NODE] = y
            marks = jnp.where(lane == n, jnp.sum(y * y), marks)
        csq[...] = marks
    csqbuf[r] = csq[...]

    def scopy(t):
        peer = lax.bitwise_xor(r, t)
        return pltpu.make_async_remote_copy(csq, csqbuf.at[r], ssend, screcv.at[r], device_id={"row": peer}, device_id_type=MESH)

    for t in range(1, nrow):
        scopy(t).start()

    unroll = 4 if panels % 4 == 0 else 1

    @pl.loop(0, panels // unroll)
    def _(b):
        for u in range(unroll):
            p = b * unroll + u
            for j in range(1, nchip):
                peer = lax.bitwise_xor(chip, j)
                xcopy(p, chip, peer, peer * 2 + core).wait_recv()
        xs, places, marks = [], [], rsq[...]
        for u in range(unroll):
            p = b * unroll + u
            x = rchip[p, 0]
            for j in range(1, nchip):
                x = x + rchip[p, j]
            xs.append(x)
            places.append(pl.ds(pl.multiple_of(p * NODE, NODE), NODE))
        ys = project(xs, [rb[where, :] for where in places])
        for u, y in enumerate(ys):
            row_out[:, places[u]] = y
            marks = jnp.where(lane == b * unroll + u, jnp.sum(y * y), marks)
        rsq[...] = marks

    rsqbuf[c] = rsq[...]

    def tcopy(s):
        peer = lax.bitwise_xor(c, s)
        return pltpu.make_async_remote_copy(rsq, rsqbuf.at[c], ssend, srrecv.at[c], device_id={"col": peer}, device_id_type=MESH)

    for s in range(1, ncol):
        tcopy(s).start()

    def wait_slot(src, buf, sems, slot, dev):
        pltpu.make_async_remote_copy(src, buf.at[slot], ssend, sems.at[slot], device_id=dev, device_id_type=MESH).wait_recv()

    lcopy(left, c, partner).wait_send()
    for j in range(1, nchip):
        lcopy(left, c, partner).wait_send()
        lcopy(leftbuf.at[c], c, partner).wait_send()
    for t in range(1, nrow):
        gcopy(r, r).wait_send()
        for h in range(2):
            ccopy(h, r, r, r).wait_send()

    @pl.loop(0, panels)
    def _(p):
        pcopy(p).wait_send()
        for j in range(1, nchip):
            xcopy(p, chip, chip, c).wait_send()

    for t in range(1, nrow):
        peer = lax.bitwise_xor(r, t)
        wait_slot(csq, csqbuf, screcv, peer, {"row": peer})
    for s in range(1, ncol):
        peer = lax.bitwise_xor(c, s)
        wait_slot(rsq, rsqbuf, srrecv, peer, {"col": peer})
    count = samples * NODE
    total = rsqbuf[0]
    for s in range(1, ncol):
        total = total + rsqbuf[s]
    rspread[...] = jnp.sqrt(total / count)
    total = csqbuf[0]
    for t in range(1, nrow):
        total = total + csqbuf[t]
    cspread[...] = jnp.sqrt(total / count)
    for t in range(1, nrow):
        scopy(t).wait_send()
    for s in range(1, ncol):
        tcopy(s).wait_send()


def shards(nrow, ncol, front, right, left, row_basis, column_basis):
    rows, cols = front.shape
    samples = right.shape[1]
    early = row_basis.shape[1]
    nchip = ncol // 2
    sr, sc = samples // ncol, samples // nrow
    panels = rows // NODE
    half = cols // 2
    dma = pltpu.SemaphoreType.DMA
    hbm = pl.BlockSpec(memory_space=pl.ANY)
    vmem = pl.BlockSpec(memory_space=pltpu.VMEM)
    row_s, col_s, rs, cs = pl.pallas_call(
        functools.partial(kernel, nrow, ncol),
        out_shape=(
            jax.ShapeDtypeStruct((sr, rows), F32),
            jax.ShapeDtypeStruct((sc, cols), F32),
            jax.ShapeDtypeStruct((8, 128), F32),
            jax.ShapeDtypeStruct((8, 128), F32),
        ),
        in_specs=[hbm] * 5,
        out_specs=(vmem,) * 4,
        scratch_shapes=[
            pltpu.VMEM((ncol,) + left.shape, BF16),
            pltpu.VMEM((nrow,) + right.shape, BF16),
            pltpu.VMEM((BUFS, rows // ncol, half), BF16),
            pltpu.VMEM((BUFS, NODE, cols), BF16),
            pltpu.VMEM((2, nrow, sc, half), F32),
            pltpu.VMEM((2, nrow, sc, half), F32),
            pltpu.VMEM((panels, 2, nchip, sr, NODE), F32),
            pltpu.VMEM((panels, nchip, sr, NODE), F32),
            pltpu.VMEM((panels, nchip, sr, NODE), F32),
            pltpu.VMEM((panels, nchip, sr, NODE), F32),
            pltpu.VMEM((rows, early), BF16),
            pltpu.VMEM((cols, early), BF16),
            pltpu.VMEM((8, 128), F32),
            pltpu.VMEM((8, 128), F32),
            pltpu.VMEM((ncol, 8, 128), F32),
            pltpu.VMEM((nrow, 8, 128), F32),
            dma, dma((ncol,)), dma, dma((nrow,)), dma, dma((2, nrow)),
            dma, dma((panels,)), dma, dma((panels, nchip)),
            dma, dma((ncol,)), dma((nrow,)), dma((2,)), dma((2,)), dma((BUFS,)), dma((BUFS,)),
        ],
        compiler_params=pltpu.CompilerParams(
            collective_id=0, has_side_effects=True, vmem_limit_bytes=62 * 1024 * 1024
        ),
    )(front, right, left, row_basis, column_basis)
    return row_s, col_s, rs[0, :rows // NODE], cs[0, :cols // NODE]


def solution(mesh):
    in_specs = (
        P("row", "col"),
        P(("col", "row"), None),
        P(("row", "col"), None),
        P("row", None),
        P("col", None),
    )
    out_specs = (P("col", "row"), P("row", "col"), P("row"), P("col"))
    body = functools.partial(shards, mesh.shape["row"], mesh.shape["col"])
    return jax.shard_map(body, mesh=mesh, in_specs=in_specs, out_specs=out_specs, check_vma=False)
```
